32 devices in a mesh: north: 4 (over y, x), east: 8 (over z, core).
Axes of the slice: x: 2, y: 2, z: 4, core: 2. Of those that a mesh axis runs over, the one named last changes fastest.
Arguments:
- pair_rows: bfloat16 [96, 96, 128], P('north', 'east'), may hold values from -6 to 6
- in_gain: float32 [128], replicated, may hold values from 0.25 to 1.75
- left_weight: bfloat16 [128, 128], replicated, may hold values from -0.5 to 0.5
- right_weight: bfloat16 [128, 128], replicated, may hold values from -0.5 to 0.5
- left_gate: bfloat16 [128, 128], replicated, may hold values from -0.5 to 0.5
- right_gate: bfloat16 [128, 128], replicated, may hold values from -0.5 to 0.5
- mid_gain: float32 [128], replicated, may hold values from 0.25 to 1.75
- out_weight: bfloat16 [128, 128], replicated, may hold values from -0.5 to 0.5
- out_gate: bfloat16 [128, 128], replicated, may hold values from -0.5 to 0.5
Outputs:
- pair_change: bfloat16 [96, 96, 128], P('north', 'east')
The draws below stay inside these ranges and needn't reach their ends.
All inputs are finite; a program needn't handle non-finite values.
Results may differ from the reference program's by a relative error of at most 0.012.
Values may be sent and summed in bfloat16 or wider, within the bound.
No kernel may reach another device: no remote copies, remote signals or barrier semaphores. Data moves between devices by JAX's collectives and lax.ppermute only.
A program may use at most 128 MiB of HBM per device.

```python
import jax
import jax.numpy as jnp
from jax import lax

RESIDUES = 96
PAIR_WIDTH = 128
MIX_WIDTH = 128


def levels(stream_key, shape, split, smallest, top_value):
    level = 1.0
    for dim, shards_of in split:
        draws = jax.random.uniform(jax.random.fold_in(jax.random.fold_in(stream_key, 6), dim), (shards_of,), jnp.float32, smallest / len(split), top_value / len(split))
        level = level * jnp.repeat(jnp.exp(draws), shape[dim] // shards_of).reshape((-1,) + (1,) * (len(shape) - 1 - dim))
    return level


def scatter_about(own_key, dims, width, most, split=(), dtype=jnp.bfloat16):
    entries = jax.random.normal(own_key, dims, jnp.float32) * width
    if len(split) > 0:
        entries = levels(own_key, dims, split, -0.22, 0.18) * entries
    return jnp.clip(entries, min=-most, max=most).astype(dtype)


def setup_inputs(seed: int = 0) -> dict:
    key_list = jax.random.split(jax.random.key(seed), 10)
    return {
        "pair_rows": scatter_about(key_list[0], (RESIDUES, RESIDUES, PAIR_WIDTH), 1.0, 6.0, ((0, 4), (1, 8))),
        "in_gain": jnp.clip(1.0 + 0.15 * jax.random.normal(key_list[1], (PAIR_WIDTH,), jnp.float32), 0.25, 1.75),
        "left_weight": scatter_about(key_list[2], (PAIR_WIDTH, MIX_WIDTH), PAIR_WIDTH ** -0.5, 0.5),
        "right_weight": scatter_about(key_list[3], (PAIR_WIDTH, MIX_WIDTH), PAIR_WIDTH ** -0.5, 0.5),
        "left_gate": scatter_about(key_list[4], (PAIR_WIDTH, MIX_WIDTH), PAIR_WIDTH ** -0.5, 0.5),
        "right_gate": scatter_about(key_list[5], (PAIR_WIDTH, MIX_WIDTH), PAIR_WIDTH ** -0.5, 0.5),
        "mid_gain": jnp.clip(1.0 + 0.15 * jax.random.normal(key_list[6], (MIX_WIDTH,), jnp.float32), 0.25, 1.75),
        "out_weight": scatter_about(key_list[7], (MIX_WIDTH, PAIR_WIDTH), MIX_WIDTH ** -0.5, 0.5),
        "out_gate": scatter_about(key_list[8], (PAIR_WIDTH, PAIR_WIDTH), PAIR_WIDTH ** -0.5, 0.5),
    }


def scale_channels(values, channel_gain):
    centred = values - lax.optimization_barrier(jnp.mean(values, axis=-1, keepdims=True))
    return centred * lax.rsqrt(lax.optimization_barrier(jnp.mean(centred * centred, axis=-1, keepdims=True)) + 1e-05) * channel_gain

def both_factors(pair_in, in_gain, left_weight, right_weight, left_gate, right_gate):
    ready = scale_channels(pair_in.astype(jnp.float32), in_gain).astype(jnp.bfloat16)
    ready = lax.optimization_barrier(ready)
    left = jnp.einsum('ijc,cd->ijd', ready.astype(jnp.float32), left_weight.astype(jnp.float32))
    left = left * jax.nn.sigmoid(jnp.einsum('ijc,cd->ijd', ready.astype(jnp.float32), left_gate.astype(jnp.float32)))
    right = jnp.einsum('ijc,cd->ijd', ready.astype(jnp.float32), right_weight.astype(jnp.float32))
    right = right * jax.nn.sigmoid(jnp.einsum('ijc,cd->ijd', ready.astype(jnp.float32), right_gate.astype(jnp.float32)))
    return (ready, left.astype(jnp.bfloat16), right.astype(jnp.bfloat16))

def to_pair(mixed, ready, mid_gain, out_weight, out_gate):
    scaled = scale_channels(mixed.astype(jnp.float32), mid_gain).astype(jnp.bfloat16)
    scaled = lax.optimization_barrier(scaled)
    gate = jax.nn.sigmoid(jnp.einsum('ijc,cd->ijd', ready.astype(jnp.float32), out_gate.astype(jnp.float32)))
    return (jnp.einsum('ijd,dc->ijc', scaled.astype(jnp.float32), out_weight.astype(jnp.float32)) * gate).astype(jnp.bfloat16)

def reference(pair_rows, in_gain, left_weight, right_weight, left_gate, right_gate, mid_gain, out_weight, out_gate):
    ready, left, right = both_factors(pair_rows, in_gain, left_weight, right_weight, left_gate, right_gate)
    left, right = lax.optimization_barrier((left, right))

    def one_channel(pair_of):
        return (jnp.dot(pair_of[0].T, pair_of[1], preferred_element_type=jnp.float32) * RESIDUES ** (-0.5)).astype(jnp.bfloat16)
    mixed = jnp.moveaxis(lax.map(one_channel, (jnp.moveaxis(left, -1, 0), jnp.moveaxis(right, -1, 0))), 0, -1)
    mixed = lax.optimization_barrier(mixed)
    return to_pair(mixed, ready, mid_gain, out_weight, out_gate)
```

```python
import functools

import jax
import jax.numpy as jnp
from jax import lax
from jax.experimental import pallas as pl
from jax.experimental.pallas import tpu as pltpu
from jax.sharding import PartitionSpec as P


F32, BF16 = jnp.float32, jnp.bfloat16
CORES = 2
VMEM = pl.BlockSpec(memory_space=pltpu.VMEM)


def scale_channels(values, channel_gain):
    centred = values - jnp.mean(values, axis=-1, keepdims=True)
    return (
        centred
        * lax.rsqrt(jnp.mean(centred * centred, axis=-1, keepdims=True) + 1e-05)
        * channel_gain
    )


def dot(a, b):
    return jnp.dot(a, b, preferred_element_type=F32)


def call(kernel, out_shape, args, flops, scratch=(), grant=8):
    outs = jax.tree.map(lambda _: VMEM, out_shape)
    size = sum(a.size * a.dtype.itemsize for a in args)
    return pl.pallas_call(
        kernel,
        out_shape=out_shape,
        in_specs=[VMEM] * len(args),
        out_specs=outs,
        scratch_shapes=list(scratch),
        cost_estimate=pl.CostEstimate(flops=flops, bytes_accessed=size, transcendentals=0),
        compiler_params=pltpu.CompilerParams(vmem_limit_bytes=grant << 20),
        name=kernel.__name__ if hasattr(kernel, "__name__") else kernel.func.__name__,
    )(*args)


def left_kernel(x_ref, gain_ref, weight_ref, gate_ref, ready_ref, left_ref):
    width, height, channels = x_ref.shape
    x = x_ref[...].astype(F32).reshape(width * height, channels)
    ready = scale_channels(x, gain_ref[...]).astype(BF16)
    ready_ref[...] = ready.reshape(width, height, channels)
    left = dot(ready, weight_ref[...]) * jax.nn.sigmoid(dot(ready, gate_ref[...]))
    left_ref[...] = left.astype(BF16).reshape(left_ref.shape)


def right_kernel(ready_ref, weight_ref, gate_ref, right_ref):
    width, height, channels = ready_ref.shape
    ready = ready_ref[...].reshape(width * height, channels)
    right = dot(ready, weight_ref[...]) * jax.nn.sigmoid(dot(ready, gate_ref[...]))
    right_ref[...] = right.astype(BF16).reshape(right_ref.shape)


def mix_kernel(levels, rows, *refs):
    where_ref, own_ref, other_ref, *lefts = refs[: 3 + levels]
    outs = refs[3 + levels : 3 + levels + rows]
    flat_ref, right_ref, left_ref = refs[3 + levels + rows :]
    width, height, channels = own_ref.shape
    both = CORES * width
    level, row = where_ref[0], where_ref[1]
    for part, ref in enumerate((own_ref, other_ref)):
        flat_ref[pl.ds(part * width * height, width * height), :] = (
            ref[...].astype(F32).reshape(width * height, channels)
        )
    for k in range(height):
        right_ref[k] = flat_ref[pl.ds(k, both, stride=height), :].reshape(both // 8, 8, channels)
    for s, ref in enumerate(lefts):
        left_ref[s] = ref[...].astype(F32).reshape(width * height, channels)

    per_row = levels // rows
    tile_j = 3 if (both // 8) % 3 == 0 else 1
    tile_i = 12 if width % 12 == 0 else 4
    step = 8

    def tile(out_ref, s, r, i0, j0):
        def some(kk, total):
            total = list(total)
            for dk in range(step):
                k = kk * step + dk
                right = right_ref[k, pl.ds(j0, tile_j)]
                for i in range(tile_i):
                    start = (i0 + i) * height + k
                    total[i] = total[i] + right * left_ref[s, pl.ds(start, 8, stride=0), :][None]
            return tuple(total)

        zero = jnp.zeros((tile_j, 8, channels), F32)
        total = lax.fori_loop(0, height // step, some, (zero,) * tile_i, unroll=height <= 24)
        for i in range(tile_i):
            out_ref[r * width + i0 + i, pl.ds(j0 * 8, tile_j * 8), :] = (
                total[i].reshape(tile_j * 8, channels).astype(out_ref.dtype)
            )

    for a, out_ref in enumerate(outs):
        target = row ^ a
        for r in range(per_row):
            s = lax.rem(level - (target * per_row + r) + levels, levels)
            for i0 in range(0, width, tile_i):
                for j0 in range(0, both // 8, tile_j):
                    tile(out_ref, s, r, i0, j0)


def mixed_kernel(scale, *refs):
    gain_ref, *parts = refs[:-2]
    keep_ref, send_ref = refs[-2:]
    total = parts[0][...].astype(F32)
    for ref in parts[1:]:
        total = total + ref[...].astype(F32)
    mixed = (total * scale).astype(BF16).astype(F32)
    rows, both, channels = mixed.shape
    scaled = scale_channels(mixed, gain_ref[...].reshape(1, 1, channels)).astype(BF16)
    keep_ref[...] = scaled[:, : both // CORES]
    send_ref[...] = scaled[:, both // CORES :]


def out_kernel(per_row, where_ref, keep_ref, come_ref, ready_ref, gate_ref, weight_ref, out_ref, flat_ref):
    width, height, channels = ready_ref.shape
    pitch = flat_ref.shape[0] // height
    core = where_ref[2]
    for r in range(per_row):
        for ref, at in ((keep_ref, core), (come_ref, 1 - core)):
            for i in range(width):
                start = ((r * CORES + at) * width + i) * pitch
                flat_ref[pl.ds(pl.multiple_of(start, 8), width), :] = ref[r * width + i].astype(F32)
    scaled = jnp.concatenate(
        [flat_ref[pl.ds(j, height, stride=pitch), :] for j in range(width)], axis=0
    ).astype(BF16)
    ready = ready_ref[...].reshape(width * height, channels)
    gate = jax.nn.sigmoid(dot(ready, gate_ref[...]))
    out = dot(scaled, weight_ref[...]) * gate
    out_ref[...] = out.astype(BF16).reshape(out_ref.shape)


def body(
    pair_rows,
    in_gain,
    left_weight,
    right_weight,
    left_gate,
    right_gate,
    mid_gain,
    out_weight,
    out_gate,
):
    rows, blocks = lax.axis_size("north"), lax.axis_size("east")
    levels = blocks // CORES
    per_row = levels // rows
    height, width, channels = pair_rows.shape
    mix_width = left_weight.shape[1]
    assert levels == per_row * rows and rows & (rows - 1) == 0 and height == per_row * CORES * width
    north, east = lax.axis_index("north"), lax.axis_index("east")
    where = jnp.stack([east // CORES, north, east % CORES]).astype(jnp.int32)
    pairs = width * height
    block = jax.ShapeDtypeStruct((width, height, mix_width), BF16)
    ready_shape = jax.ShapeDtypeStruct((width, height, channels), BF16)

    def along(axis, size, target, value):
        return lax.ppermute(value, axis, [(i, target(i)) for i in range(size)])

    def shifted(value, s):
        return along("east", blocks, lambda e: (e + s * CORES) % blocks, value)

    x = jnp.transpose(pair_rows, (1, 0, 2))
    gain = in_gain.reshape(1, channels)
    flops = 4 * pairs * channels * mix_width
    ready, left = call(
        left_kernel, (ready_shape, block), (x, gain, left_weight, left_gate), flops
    )
    lefts = [left] + [shifted(left, s) for s in range(1, levels)]
    right = call(right_kernel, block, (ready, right_weight, right_gate), flops)
    other = along("east", blocks, lambda e: e ^ 1, right)

    both = CORES * width
    part_rows = per_row * width
    parts = tuple(
        jax.ShapeDtypeStruct((part_rows, both, mix_width), BF16 if a else F32) for a in range(rows)
    )
    smem = pl.BlockSpec(memory_space=pltpu.SMEM)
    mix = functools.partial(mix_kernel, levels, rows)
    parts = pl.pallas_call(
        mix,
        out_shape=parts,
        in_specs=[smem] + [VMEM] * (2 + levels),
        out_specs=(VMEM,) * rows,
        scratch_shapes=[
            pltpu.VMEM((both * height, mix_width), F32),
            pltpu.VMEM((height, both // 8, 8, mix_width), F32),
            pltpu.VMEM((levels, pairs, mix_width), F32),
        ],
        cost_estimate=pl.CostEstimate(
            flops=2 * rows * part_rows * both * height * mix_width, bytes_accessed=0, transcendentals=0
        ),
        compiler_params=pltpu.CompilerParams(vmem_limit_bytes=(8 << 20) + 6 * levels * pairs * mix_width * 2),
        name="mix_kernel",
    )(where, right, other, *lefts)
    arrived = [parts[0]] + [
        along("north", rows, lambda n: n ^ a, parts[a]) for a in range(1, rows)
    ]

    half = jax.ShapeDtypeStruct((part_rows, width, mix_width), BF16)
    scale = (height * rows) ** (-0.5)
    keep, send = call(
        functools.partial(mixed_kernel, scale),
        (half, half),
        (mid_gain.reshape(1, mix_width), *arrived),
        4 * pairs * mix_width,
        grant=24,
    )
    come = along("east", blocks, lambda e: e ^ 1, send)
    pitch = -(-width // 8) * 8
    out = pl.pallas_call(
        functools.partial(out_kernel, per_row),
        out_shape=ready_shape,
        in_specs=[smem] + [VMEM] * 5,
        out_specs=VMEM,
        scratch_shapes=[pltpu.VMEM((height * pitch, mix_width), F32)],
        cost_estimate=pl.CostEstimate(flops=flops, bytes_accessed=0, transcendentals=0),
        compiler_params=pltpu.CompilerParams(vmem_limit_bytes=24 << 20),
        name="out_kernel",
    )(where, keep, come, ready, out_gate, out_weight)
    return jnp.transpose(out, (1, 0, 2))


def solution(mesh):
    placed = (P("north", "east", None), P(), P(), P(), P(), P(), P(), P(), P())
    return jax.shard_map(
        body, mesh=mesh, in_specs=placed, out_specs=P("north", "east", None), check_vma=False
    )
```

```python
import math

import jax
import jax.numpy as jnp
from jax import lax
from jax.experimental import pallas as pl
from jax.experimental.pallas import tpu as pltpu
from jax.sharding import PartitionSpec as P


F32, BF16 = jnp.float32, jnp.bfloat16
CORES = 2
VMEM = pl.BlockSpec(memory_space=pltpu.VMEM)
HBM = pl.BlockSpec(memory_space=pltpu.HBM)


def scale_channels(values, channel_gain):
    centred = values - jnp.mean(values, axis=-1, keepdims=True)
    return (
        centred
        * lax.rsqrt(jnp.mean(centred * centred, axis=-1, keepdims=True) + 1e-05)
        * channel_gain
    )


def dot(a, b):
    return jnp.dot(a, b, preferred_element_type=F32)


def shape(dims, dtype=BF16):
    return jax.ShapeDtypeStruct(tuple(dims), dtype)


def call(kernel, outs, specs, args, us, scratch=()):
    tree = jax.tree.map(lambda _: VMEM, outs)
    live = sum(math.prod(a.shape) * a.dtype.itemsize for a in (*jax.tree.leaves(outs), *args))
    live += sum(math.prod(s.shape) * 4 for s in scratch if s.memory_space == pltpu.VMEM)
    return pl.pallas_call(
        kernel,
        out_shape=outs,
        in_specs=specs,
        out_specs=tree,
        scratch_shapes=list(scratch),
        cost_estimate=pl.CostEstimate(flops=int(us * 16e6), bytes_accessed=0, transcendentals=0),
        compiler_params=pltpu.CompilerParams(vmem_limit_bytes=min((8 << 20) + 2 * live, 60 << 20)),
    )(*args)


def ready_of(x_ref, gain):
    width, height, channels = x_ref.shape
    x = x_ref[...].astype(F32).reshape(width * height, channels)
    return scale_channels(x, gain).astype(BF16)


def gated(ready, weight_ref, gate_ref):
    return (dot(ready, weight_ref[...]) * jax.nn.sigmoid(dot(ready, gate_ref[...]))).astype(BF16)


def own_kernel(n_copies, pitch, *refs):
    x_hbm, og_hbm = refs[:2]
    sources = refs[2 : 2 + n_copies]
    ready_ref, gate_ref, right_ref, turn_ref = refs[2 + n_copies : 6 + n_copies]
    copies = refs[6 + n_copies : 6 + 2 * n_copies]
    x_ref, og_ref, sems = refs[6 + 2 * n_copies :]
    moves = [
        pltpu.make_async_copy(source, target, sems.at[i])
        for i, (source, target) in enumerate(
            zip((x_hbm, og_hbm, *sources), (x_ref, og_ref, *copies), strict=True)
        )
    ]
    for move in moves:
        move.start()
    width, height, _ = x_ref.shape
    columns = turn_ref.shape[2]
    core = lax.rem(lax.axis_index("east"), CORES)
    row = lax.broadcasted_iota(jnp.int32, (height, columns), 0)
    column = lax.broadcasted_iota(jnp.int32, (height, columns), 1)
    for half in range(CORES):
        offset = half * (pitch - width)
        at = core if half == 0 else 1 - core
        for j in range(width):
            hit = jnp.zeros((height, columns), F32)
            for r in range(height // (CORES * width)):
                first = (r * CORES + at) * width
                inside = (row >= first) & (row < first + width)
                same = column == (row - first + r * width) * pitch + (j + offset)
                hit = jnp.where(inside & same, 1.0, hit)
            turn_ref[half, pl.ds(j * height, height), :] = hit.astype(BF16)
    for move in moves:
        move.wait()
    gain_ref, _, _, _, rw_ref, rg_ref, _ = copies
    ready = ready_of(x_ref, gain_ref[...])
    ready_ref[...] = ready
    gate_ref[...] = jax.nn.sigmoid(dot(ready, og_ref[...]))
    right_ref[...] = gated(ready, rw_ref, rg_ref).astype(F32)


def mix(out_ref, left_ref, right_ref):
    height, tiles_j, _, channels = right_ref.shape
    width = out_ref.shape[0]
    tile_j = 3 if tiles_j % 3 == 0 else 1
    tile_i = 12 if width % 12 == 0 else 4
    step = 8
    for i0 in range(0, width, tile_i):
        for j0 in range(0, tiles_j, tile_j):

            def some(kk, total, i0=i0, j0=j0):
                total = list(total)
                for dk in range(step):
                    k = kk * step + dk
                    right = right_ref[k, pl.ds(j0, tile_j)]
                    for i in range(tile_i):
                        start = (i0 + i) * height + k
                        total[i] = total[i] + right * left_ref[pl.ds(start, 8, stride=0), :][None]
                return tuple(total)

            zero = jnp.zeros((tile_j, 8, channels), F32)
            total = lax.fori_loop(0, height // step, some, (zero,) * tile_i, unroll=height <= 24)
            for i in range(tile_i):
                out_ref[i0 + i, pl.ds(j0 * 8, tile_j * 8), :] = (
                    total[i].reshape(tile_j * 8, channels).astype(BF16)
                )


def first_kernel(
    x_ref, gain_ref, lw_ref, lg_ref, rw_ref, rg_ref, ready_ref, own_ref, right_ref, part_ref, flat_ref, left_ref
):
    pairs = own_ref.shape[0]
    height, tiles_j, _, channels = right_ref.shape
    flat_ref[pl.ds(0, pairs), :] = own_ref[...]
    other = gated(ready_of(x_ref, gain_ref[...]), rw_ref, rg_ref)
    flat_ref[pl.ds(pairs, pairs), :] = other.astype(F32)
    for k in range(height):
        right_ref[k] = flat_ref[pl.ds(k, tiles_j * 8, stride=height), :].reshape(tiles_j, 8, channels)
    left_ref[...] = gated(ready_ref[...], lw_ref, lg_ref).astype(F32)
    mix(part_ref, left_ref, right_ref)


def next_kernel(x_ref, gain_ref, lw_ref, lg_ref, right_ref, part_ref, left_ref):
    left_ref[...] = gated(ready_of(x_ref, gain_ref[...]), lw_ref, lg_ref).astype(F32)
    mix(part_ref, left_ref, right_ref)


def last_kernel(levels, rows, *refs):
    x_ref, gain_ref, lw_ref, lg_ref, right_ref = refs[:5]
    parts = refs[5 : 4 + levels]
    outs = refs[4 + levels : 4 + levels + rows]
    all_ref, left_ref = refs[4 + levels + rows :]
    level, row = lax.div(lax.axis_index("east"), CORES), lax.axis_index("north")
    left_ref[...] = gated(ready_of(x_ref, gain_ref[...]), lw_ref, lg_ref).astype(F32)
    mix(all_ref.at[levels - 1], left_ref, right_ref)
    for s, ref in enumerate(parts):
        all_ref[s] = ref[...]
    per_row = levels // rows
    width = all_ref.shape[1]
    for a, out_ref in enumerate(outs):
        for r in range(per_row):
            s = lax.rem(level - ((row ^ a) * per_row + r) + levels, levels)
            out_ref[pl.ds(r * width, width)] = all_ref[s]


def sum_kernel(scale, gain_ref, *refs):
    parts, (keep_ref, send_ref) = refs[:-2], refs[-2:]
    total = parts[0][...].astype(F32)
    for ref in parts[1:]:
        total = total + ref[...].astype(F32)
    mixed = (total * scale).astype(BF16).astype(F32)
    channels = mixed.shape[2]
    scaled = scale_channels(mixed, gain_ref[...].reshape(1, 1, channels)).astype(BF16)
    pitch = keep_ref.shape[1]
    keep_ref[...] = scaled[:, :pitch]
    send_ref[...] = scaled[:, scaled.shape[1] - pitch :]


def turned(half_ref, turn_ref, which, weight_ref):
    rows, pitch, channels = half_ref.shape
    half = half_ref[...].reshape(rows * pitch, channels)
    return dot(dot(turn_ref[which], half).astype(BF16), weight_ref[...])


def keep_kernel(keep_ref, turn_ref, weight_ref, out_ref):
    out_ref[...] = turned(keep_ref, turn_ref, 0, weight_ref)


def out_kernel(come_ref, turn_ref, weight_ref, kept_ref, gate_ref, out_ref):
    out = (kept_ref[...] + turned(come_ref, turn_ref, 1, weight_ref)) * gate_ref[...]
    out_ref[...] = out.astype(BF16).reshape(out_ref.shape)


def body(
    pair_rows,
    in_gain,
    left_weight,
    right_weight,
    left_gate,
    right_gate,
    mid_gain,
    out_weight,
    out_gate,
):
    rows, blocks = lax.axis_size("north"), lax.axis_size("east")
    levels = blocks // CORES
    per_row = levels // rows
    height, width, channels = pair_rows.shape
    mix_width = left_weight.shape[1]
    both, pairs, part_rows = CORES * width, width * height, per_row * width
    pitch = both - width // 8 * 8
    assert levels == per_row * rows and rows & (rows - 1) == 0 and height == per_row * both
    assert both % 8 == 0 and height % 8 == 0 and pitch % 8 == 0

    def along(axis, size, target, value):
        return lax.ppermute(value, axis, [(i, target(i)) for i in range(size)])

    x = jnp.transpose(pair_rows, (1, 0, 2))
    far = [
        along("east", blocks, lambda e, s=s: (e + s * CORES) % blocks, x)
        for s in range(1, levels)
    ]
    beside = along("east", blocks, lambda e: e ^ 1, x)

    copied = (
        in_gain.reshape(1, channels),
        mid_gain.reshape(1, mix_width),
        left_weight,
        left_gate,
        right_weight,
        right_gate,
        out_weight,
    )
    n = len(copied)
    ready, gate, own_right, turn, gain, mid, lw, lg, rw, rg, ow = call(
        lambda *refs: own_kernel(n, pitch, *refs),
        (
            shape((pairs, channels)),
            shape((pairs, channels), F32),
            shape((pairs, mix_width), F32),
            shape((CORES, pairs, part_rows * pitch)),
            *(shape(a.shape, a.dtype) for a in copied),
        ),
        [HBM] * (2 + n),
        [pltpu.with_memory_space_constraint(a, pltpu.HBM) for a in (x, out_gate, *copied)],
        1.5,
        [
            pltpu.VMEM(x.shape, BF16),
            pltpu.VMEM(out_gate.shape, BF16),
            pltpu.SemaphoreType.DMA((2 + n,)),
        ],
    )

    part = shape((width, both, mix_width))
    flat = pltpu.VMEM((pairs, mix_width), F32)
    right, own_part = call(
        first_kernel,
        (shape((height, both // 8, 8, mix_width), F32), part),
        [VMEM] * 8,
        (beside, gain, lw, lg, rw, rg, ready, own_right),
        1.0,
        [pltpu.VMEM((both * height, mix_width), F32), flat],
    )
    parts = [own_part]
    for s in range(1, levels - 1):
        parts.append(
            call(next_kernel, part, [VMEM] * 5, (far[s - 1], gain, lw, lg, right), 0.6, [flat])
        )
    sums = call(
        lambda *refs: last_kernel(levels, rows, *refs),
        (shape((part_rows, both, mix_width)),) * rows,
        [VMEM] * (4 + levels),
        (far[-1], gain, lw, lg, right, *parts),
        0.8,
        [pltpu.VMEM((levels, width, both, mix_width), BF16), flat],
    )
    arrived = [sums[0]] + [
        along("north", rows, lambda n, a=a: n ^ a, sums[a]) for a in range(1, rows)
    ]

    half = shape((part_rows, pitch, mix_width))
    scale = (height * rows) ** (-0.5)
    keep, send = call(
        lambda *refs: sum_kernel(scale, *refs),
        (half, half),
        [VMEM] * (1 + rows),
        (mid, *arrived),
        0.3,
    )
    come = along("east", blocks, lambda e: e ^ 1, send)
    kept = call(keep_kernel, shape((pairs, channels), F32), [VMEM] * 3, (keep, turn, ow), 0.3)
    out = call(
        out_kernel, shape((width, height, channels)), [VMEM] * 5, (come, turn, ow, kept, gate), 0.5
    )
    return jnp.transpose(out, (1, 0, 2))


def solution(mesh):
    placed = (P("north", "east", None), P(), P(), P(), P(), P(), P(), P(), P())

    return jax.shard_map(
        body, mesh=mesh, in_specs=placed, out_specs=P("north", "east", None), check_vma=False
    )
```

```python
import math

import jax
import jax.numpy as jnp
from jax import lax
from jax.experimental import pallas as pl
from jax.experimental.pallas import tpu as pltpu
from jax.sharding import PartitionSpec as P


F32, BF16 = jnp.float32, jnp.bfloat16
CORES = 2
VMEM = pl.BlockSpec(memory_space=pltpu.VMEM)
HBM = pl.BlockSpec(memory_space=pltpu.HBM)


def scale_channels(values, channel_gain):
    centred = values - jnp.mean(values, axis=-1, keepdims=True)
    return (
        centred
        * lax.rsqrt(jnp.mean(centred * centred, axis=-1, keepdims=True) + 1e-05)
        * channel_gain
    )


def dot(a, b):
    return jnp.dot(a, b, preferred_element_type=F32)


def shape(dims, dtype=BF16):
    return jax.ShapeDtypeStruct(tuple(dims), dtype)


def call(kernel, outs, specs, args, us, scratch=()):
    tree = jax.tree.map(lambda _: VMEM, outs)
    live = sum(math.prod(a.shape) * a.dtype.itemsize for a in (*jax.tree.leaves(outs), *args))
    live += sum(math.prod(s.shape) * 4 for s in scratch if s.memory_space == pltpu.VMEM)
    return pl.pallas_call(
        kernel,
        out_shape=outs,
        in_specs=specs,
        out_specs=tree,
        scratch_shapes=list(scratch),
        cost_estimate=pl.CostEstimate(flops=int(us * 16e6), bytes_accessed=0, transcendentals=0),
        compiler_params=pltpu.CompilerParams(vmem_limit_bytes=min((8 << 20) + 2 * live, 60 << 20)),
    )(*args)


def ready_of(x_ref, gain):
    width, height, channels = x_ref.shape
    x = x_ref[...].astype(F32).reshape(width * height, channels)
    return scale_channels(x, gain).astype(BF16)


def gated(ready, weight_ref, gate_ref):
    return (dot(ready, weight_ref[...]) * jax.nn.sigmoid(dot(ready, gate_ref[...]))).astype(BF16)


def own_kernel(n_copies, pitch, *refs):
    x_hbm, og_hbm = refs[:2]
    sources = refs[2 : 2 + n_copies]
    ready_ref, gate_ref, right_ref, turn_ref = refs[2 + n_copies : 6 + n_copies]
    copies = refs[6 + n_copies : 6 + 2 * n_copies]
    x_ref, og_ref, sems = refs[6 + 2 * n_copies :]
    moves = [
        pltpu.make_async_copy(source, target, sems.at[i])
        for i, (source, target) in enumerate(
            zip((x_hbm, og_hbm, *sources), (x_ref, og_ref, *copies), strict=True)
        )
    ]
    for move in moves:
        move.start()
    width, height, _ = x_ref.shape
    columns = turn_ref.shape[2]
    core = lax.rem(lax.axis_index("east"), CORES)
    row = lax.broadcasted_iota(jnp.int32, (height, columns), 0)
    column = lax.broadcasted_iota(jnp.int32, (height, columns), 1)
    for half in range(CORES):
        offset = half * (pitch - width)
        at = core if half == 0 else 1 - core
        for j in range(width):
            hit = jnp.zeros((height, columns), F32)
            for r in range(height // (CORES * width)):
                first = (r * CORES + at) * width
                inside = (row >= first) & (row < first + width)
                same = column == (row - first + r * width) * pitch + (j + offset)
                hit = jnp.where(inside & same, 1.0, hit)
            turn_ref[half, pl.ds(j * height, height), :] = hit.astype(BF16)
    for move in moves:
        move.wait()
    gain_ref, _, _, _, rw_ref, rg_ref, _ = copies
    ready = ready_of(x_ref, gain_ref[...])
    ready_ref[...] = ready
    gate_ref[...] = jax.nn.sigmoid(dot(ready, og_ref[...]))
    right_ref[...] = gated(ready, rw_ref, rg_ref).astype(F32)


def mix(out_ref, left_ref, right_ref):
    height, tiles_j, _, channels = right_ref.shape
    width = out_ref.shape[0]
    tile_j = 3 if tiles_j % 3 == 0 else 1
    tile_i = 12 if width % 12 == 0 else 4
    step = 8
    for i0 in range(0, width, tile_i):
        for j0 in range(0, tiles_j, tile_j):

            def some(kk, total, i0=i0, j0=j0):
                total = list(total)
                for dk in range(step):
                    k = kk * step + dk
                    right = right_ref[k, pl.ds(j0, tile_j)]
                    for i in range(tile_i):
                        start = (i0 + i) * height + k
                        total[i] = total[i] + right * left_ref[pl.ds(start, 8, stride=0), :][None]
                return tuple(total)

            zero = jnp.zeros((tile_j, 8, channels), F32)
            total = lax.fori_loop(0, height // step, some, (zero,) * tile_i, unroll=height <= 24)
            for i in range(tile_i):
                out_ref[i0 + i, pl.ds(j0 * 8, tile_j * 8), :] = (
                    total[i].reshape(tile_j * 8, channels).astype(BF16)
                )


def first_kernel(
    x_ref, gain_ref, lw_ref, lg_ref, rw_ref, rg_ref, ready_ref, own_ref, right_ref, part_ref, flat_ref, left_ref
):
    pairs = own_ref.shape[0]
    height, tiles_j, _, channels = right_ref.shape
    flat_ref[pl.ds(0, pairs), :] = own_ref[...]
    other = gated(ready_of(x_ref, gain_ref[...]), rw_ref, rg_ref)
    flat_ref[pl.ds(pairs, pairs), :] = other.astype(F32)
    for k in range(height):
        right_ref[k] = flat_ref[pl.ds(k, tiles_j * 8, stride=height), :].reshape(tiles_j, 8, channels)
    left_ref[...] = gated(ready_ref[...], lw_ref, lg_ref).astype(F32)
    mix(part_ref, left_ref, right_ref)


def next_kernel(x_ref, gain_ref, lw_ref, lg_ref, right_ref, part_ref, left_ref):
    left_ref[...] = gated(ready_of(x_ref, gain_ref[...]), lw_ref, lg_ref).astype(F32)
    mix(part_ref, left_ref, right_ref)


def last_kernel(shifts, rows, *refs):
    levels = len(shifts)
    x_ref, gain_ref, lw_ref, lg_ref, right_ref = refs[:5]
    parts = refs[5 : 4 + levels]
    outs = refs[4 + levels : 4 + levels + rows]
    all_ref, left_ref = refs[4 + levels + rows :]
    level, row = lax.div(lax.axis_index("east"), CORES), lax.axis_index("north")
    left_ref[...] = gated(ready_of(x_ref, gain_ref[...]), lw_ref, lg_ref).astype(F32)
    mix(all_ref.at[levels - 1], left_ref, right_ref)
    for s, ref in enumerate(parts):
        all_ref[s] = ref[...]
    per_row = levels // rows
    width = all_ref.shape[1]
    for a, out_ref in enumerate(outs):
        for r in range(per_row):
            shift = level ^ ((row ^ a) * per_row + r)
            s = sum(jnp.where(shift == v, at, 0) for at, v in enumerate(shifts))
            out_ref[pl.ds(r * width, width)] = all_ref[s]


def sum_kernel(scale, gain_ref, *refs):
    parts, (keep_ref, send_ref) = refs[:-2], refs[-2:]
    total = parts[0][...].astype(F32)
    for ref in parts[1:]:
        total = total + ref[...].astype(F32)
    mixed = (total * scale).astype(BF16).astype(F32)
    channels = mixed.shape[2]
    scaled = scale_channels(mixed, gain_ref[...].reshape(1, 1, channels)).astype(BF16)
    pitch = keep_ref.shape[1]
    keep_ref[...] = scaled[:, :pitch]
    send_ref[...] = scaled[:, scaled.shape[1] - pitch :]


def turned(half_ref, turn_ref, which, weight_ref):
    rows, pitch, channels = half_ref.shape
    half = half_ref[...].reshape(rows * pitch, channels)
    return dot(dot(turn_ref[which], half).astype(BF16), weight_ref[...])


def keep_kernel(keep_ref, turn_ref, weight_ref, out_ref):
    out_ref[...] = turned(keep_ref, turn_ref, 0, weight_ref)


def out_kernel(come_ref, turn_ref, weight_ref, kept_ref, gate_ref, out_ref):
    out = (kept_ref[...] + turned(come_ref, turn_ref, 1, weight_ref)) * gate_ref[...]
    out_ref[...] = out.astype(BF16).reshape(out_ref.shape)


def body(
    pair_rows,
    in_gain,
    left_weight,
    right_weight,
    left_gate,
    right_gate,
    mid_gain,
    out_weight,
    out_gate,
):
    rows, blocks = lax.axis_size("north"), lax.axis_size("east")
    levels = blocks // CORES
    per_row = levels // rows
    height, width, channels = pair_rows.shape
    mix_width = left_weight.shape[1]
    both, pairs, part_rows = CORES * width, width * height, per_row * width
    pitch = both - width // 8 * 8
    assert levels == per_row * rows and levels & (levels - 1) == 0 and height == per_row * both
    assert both % 8 == 0 and height % 8 == 0 and pitch % 8 == 0

    def along(axis, size, target, value):
        return lax.ppermute(value, axis, [(i, target(i)) for i in range(size)])

    shifts = (0, levels - 1, *range(1, levels - 1))
    x = jnp.transpose(pair_rows, (1, 0, 2))
    far = [
        along("east", blocks, lambda e, shift=shift: e ^ (shift * CORES), x)
        for at, shift in enumerate(shifts)
        if at
    ]
    beside = along("east", blocks, lambda e: e ^ 1, x)

    copied = (
        in_gain.reshape(1, channels),
        mid_gain.reshape(1, mix_width),
        left_weight,
        left_gate,
        right_weight,
        right_gate,
        out_weight,
    )
    n = len(copied)
    ready, gate, own_right, turn, gain, mid, lw, lg, rw, rg, ow = call(
        lambda *refs: own_kernel(n, pitch, *refs),
        (
            shape((pairs, channels)),
            shape((pairs, channels), F32),
            shape((pairs, mix_width), F32),
            shape((CORES, pairs, part_rows * pitch)),
            *(shape(a.shape, a.dtype) for a in copied),
        ),
        [HBM] * (2 + n),
        [pltpu.with_memory_space_constraint(a, pltpu.HBM) for a in (x, out_gate, *copied)],
        1.5,
        [
            pltpu.VMEM(x.shape, BF16),
            pltpu.VMEM(out_gate.shape, BF16),
            pltpu.SemaphoreType.DMA((2 + n,)),
        ],
    )

    part = shape((width, both, mix_width))
    flat = pltpu.VMEM((pairs, mix_width), F32)
    right, own_part = call(
        first_kernel,
        (shape((height, both // 8, 8, mix_width), F32), part),
        [VMEM] * 8,
        (beside, gain, lw, lg, rw, rg, ready, own_right),
        1.0,
        [pltpu.VMEM((both * height, mix_width), F32), flat],
    )
    parts = [own_part]
    for s in range(1, levels - 1):
        parts.append(
            call(next_kernel, part, [VMEM] * 5, (far[s - 1], gain, lw, lg, right), 0.6, [flat])
        )
    sums = call(
        lambda *refs: last_kernel(shifts, rows, *refs),
        (shape((part_rows, both, mix_width)),) * rows,
        [VMEM] * (4 + levels),
        (far[-1], gain, lw, lg, right, *parts),
        0.8,
        [pltpu.VMEM((levels, width, both, mix_width), BF16), flat],
    )
    arrived = [sums[0]] + [
        along("north", rows, lambda n, a=a: n ^ a, sums[a]) for a in range(1, rows)
    ]

    half = shape((part_rows, pitch, mix_width))
    scale = (height * rows) ** (-0.5)
    keep, send = call(
        lambda *refs: sum_kernel(scale, *refs),
        (half, half),
        [VMEM] * (1 + rows),
        (mid, *arrived),
        0.3,
    )
    come = along("east", blocks, lambda e: e ^ 1, send)
    kept = call(keep_kernel, shape((pairs, channels), F32), [VMEM] * 3, (keep, turn, ow), 0.3)
    out = call(
        out_kernel, shape((width, height, channels)), [VMEM] * 5, (come, turn, ow, kept, gate), 0.5
    )
    return jnp.transpose(out, (1, 0, 2))


def solution(mesh):
    placed = (P("north", "east", None), P(), P(), P(), P(), P(), P(), P(), P())

    return jax.shard_map(
        body, mesh=mesh, in_specs=placed, out_specs=P("north", "east", None), check_vma=False
    )
```

```python
import math

import jax
import jax.numpy as jnp
from jax import lax
from jax.experimental import pallas as pl
from jax.experimental.pallas import tpu as pltpu
from jax.sharding import PartitionSpec as P


F32, BF16 = jnp.float32, jnp.bfloat16
CORES = 2
VMEM = pl.BlockSpec(memory_space=pltpu.VMEM)
HBM = pl.BlockSpec(memory_space=pltpu.HBM)


def scale_channels(values, channel_gain):
    centred = values - jnp.mean(values, axis=-1, keepdims=True)
    return (
        centred
        * lax.rsqrt(jnp.mean(centred * centred, axis=-1, keepdims=True) + 1e-05)
        * channel_gain
    )


def dot(a, b):
    return jnp.dot(a, b, preferred_element_type=F32)


def shape(dims, dtype=BF16):
    return jax.ShapeDtypeStruct(tuple(dims), dtype)


def call(kernel, outs, specs, args, us, scratch=()):
    tree = jax.tree.map(lambda _: VMEM, outs)
    live = sum(math.prod(a.shape) * a.dtype.itemsize for a in (*jax.tree.leaves(outs), *args))
    live += sum(math.prod(s.shape) * 4 for s in scratch if s.memory_space == pltpu.VMEM)
    return pl.pallas_call(
        kernel,
        out_shape=outs,
        in_specs=specs,
        out_specs=tree,
        scratch_shapes=list(scratch),
        cost_estimate=pl.CostEstimate(flops=int(us * 16e6), bytes_accessed=0, transcendentals=0),
        compiler_params=pltpu.CompilerParams(vmem_limit_bytes=min((8 << 20) + 2 * live, 60 << 20)),
    )(*args)


def ready_of(x_ref, gain):
    width, height, channels = x_ref.shape
    x = x_ref[...].astype(F32).reshape(width * height, channels)
    return scale_channels(x, gain).astype(BF16)


def gated(ready, weight_ref, gate_ref):
    return (dot(ready, weight_ref[...]) * jax.nn.sigmoid(dot(ready, gate_ref[...]))).astype(BF16)


def own_kernel(n_copies, pitch, *refs):
    x_hbm, og_hbm = refs[:2]
    sources = refs[2 : 2 + n_copies]
    ready_ref, gate_ref, right_ref, turn_ref = refs[2 + n_copies : 6 + n_copies]
    copies = refs[6 + n_copies : 6 + 2 * n_copies]
    x_ref, og_ref, sems = refs[6 + 2 * n_copies :]
    moves = [
        pltpu.make_async_copy(source, target, sems.at[i])
        for i, (source, target) in enumerate(
            zip((x_hbm, og_hbm, *sources), (x_ref, og_ref, *copies), strict=True)
        )
    ]
    for move in moves:
        move.start()
    width, height, _ = x_ref.shape
    columns = turn_ref.shape[2]
    level, core = lax.div(lax.axis_index("east"), CORES), lax.rem(lax.axis_index("east"), CORES)
    per_row = height // (CORES * width)
    row = lax.broadcasted_iota(jnp.int32, (height, columns), 0)
    column = lax.broadcasted_iota(jnp.int32, (height, columns), 1)
    for half in range(CORES):
        offset = half * (pitch - width)
        for j in range(width):
            hit = jnp.zeros((height, columns), F32)
            for r in range(per_row):
                near = level == lax.axis_index("north") * per_row + r
                at = jnp.where(near, 1 - core, core) if half == 0 else jnp.where(near, core, 1 - core)
                first = (r * CORES + at) * width
                inside = (row >= first) & (row < first + width)
                same = column == (row - first + r * width) * pitch + (j + offset)
                hit = jnp.where(inside & same, 1.0, hit)
            turn_ref[half, pl.ds(j * height, height), :] = hit.astype(BF16)
    for move in moves:
        move.wait()
    gain_ref, _, _, _, rw_ref, rg_ref, _ = copies
    ready = ready_of(x_ref, gain_ref[...])
    ready_ref[...] = ready
    gate_ref[...] = jax.nn.sigmoid(dot(ready, og_ref[...]))
    right_ref[...] = gated(ready, rw_ref, rg_ref).astype(F32)


def mix(out_ref, left_ref, right_ref):
    height, tiles_j, _, channels = right_ref.shape
    width = out_ref.shape[0]
    tile_j = 3 if tiles_j % 3 == 0 else 1
    tile_i = 12 if width % 12 == 0 else 4
    step = 8
    for i0 in range(0, width, tile_i):
        for j0 in range(0, tiles_j, tile_j):

            def some(kk, total, i0=i0, j0=j0):
                total = list(total)
                for dk in range(step):
                    k = kk * step + dk
                    right = right_ref[k, pl.ds(j0, tile_j)]
                    for i in range(tile_i):
                        start = (i0 + i) * height + k
                        total[i] = total[i] + right * left_ref[pl.ds(start, 8, stride=0), :][None]
                return tuple(total)

            zero = jnp.zeros((tile_j, 8, channels), F32)
            total = lax.fori_loop(0, height // step, some, (zero,) * tile_i, unroll=height <= 24)
            for i in range(tile_i):
                out_ref[i0 + i, pl.ds(j0 * 8, tile_j * 8), :] = (
                    total[i].reshape(tile_j * 8, channels).astype(BF16)
                )


def first_kernel(
    x_ref, gain_ref, lw_ref, lg_ref, rw_ref, rg_ref, ready_ref, own_ref, right_ref, part_ref, flat_ref, left_ref
):
    pairs = own_ref.shape[0]
    height, tiles_j, _, channels = right_ref.shape
    other = gated(ready_of(x_ref, gain_ref[...]), rw_ref, rg_ref)
    flat_ref[pl.ds(0, pairs), :] = other.astype(F32)
    flat_ref[pl.ds(pairs, pairs), :] = own_ref[...]
    for k in range(height):
        right_ref[k] = flat_ref[pl.ds(k, tiles_j * 8, stride=height), :].reshape(tiles_j, 8, channels)
    left_ref[...] = gated(ready_ref[...], lw_ref, lg_ref).astype(F32)
    mix(part_ref, left_ref, right_ref)


def next_kernel(x_ref, gain_ref, lw_ref, lg_ref, right_ref, part_ref, left_ref):
    left_ref[...] = gated(ready_of(x_ref, gain_ref[...]), lw_ref, lg_ref).astype(F32)
    mix(part_ref, left_ref, right_ref)


def last_kernel(shifts, rows, *refs):
    levels = len(shifts)
    x_ref, gain_ref, lw_ref, lg_ref, right_ref = refs[:5]
    parts = refs[5 : 4 + levels]
    outs = refs[4 + levels : 4 + levels + rows]
    all_ref, left_ref = refs[4 + levels + rows :]
    level, row = lax.div(lax.axis_index("east"), CORES), lax.axis_index("north")
    left_ref[...] = gated(ready_of(x_ref, gain_ref[...]), lw_ref, lg_ref).astype(F32)
    mix(all_ref.at[levels - 1], left_ref, right_ref)
    for s, ref in enumerate(parts):
        all_ref[s] = ref[...]
    per_row = levels // rows
    width = all_ref.shape[1]
    for a, out_ref in enumerate(outs):
        for r in range(per_row):
            shift = level ^ ((row ^ a) * per_row + r)
            s = sum(jnp.where(shift == v, at, 0) for at, v in enumerate(shifts))
            out_ref[pl.ds(r * width, width)] = all_ref[s]


def sum_kernel(scale, gain_ref, *refs):
    parts, (keep_ref, send_ref) = refs[:-2], refs[-2:]
    total = parts[0][...].astype(F32)
    for ref in parts[1:]:
        total = total + ref[...].astype(F32)
    mixed = (total * scale).astype(BF16).astype(F32)
    channels = mixed.shape[2]
    scaled = scale_channels(mixed, gain_ref[...].reshape(1, 1, channels)).astype(BF16)
    pitch = keep_ref.shape[1]
    keep_ref[...] = scaled[:, :pitch]
    send_ref[...] = scaled[:, scaled.shape[1] - pitch :]


def turned(half_ref, turn_ref, which, weight_ref):
    rows, pitch, channels = half_ref.shape
    half = half_ref[...].reshape(rows * pitch, channels)
    return dot(dot(turn_ref[which], half).astype(BF16), weight_ref[...])


def keep_kernel(keep_ref, turn_ref, weight_ref, out_ref):
    out_ref[...] = turned(keep_ref, turn_ref, 0, weight_ref)


def out_kernel(come_ref, turn_ref, weight_ref, kept_ref, gate_ref, out_ref):
    out = (kept_ref[...] + turned(come_ref, turn_ref, 1, weight_ref)) * gate_ref[...]
    out_ref[...] = out.astype(BF16).reshape(out_ref.shape)


def body(
    pair_rows,
    in_gain,
    left_weight,
    right_weight,
    left_gate,
    right_gate,
    mid_gain,
    out_weight,
    out_gate,
):
    rows, blocks = lax.axis_size("north"), lax.axis_size("east")
    levels = blocks // CORES
    per_row = levels // rows
    height, width, channels = pair_rows.shape
    mix_width = left_weight.shape[1]
    both, pairs, part_rows = CORES * width, width * height, per_row * width
    pitch = both - width // 8 * 8
    assert levels == per_row * rows and levels & (levels - 1) == 0 and height == per_row * both
    assert both % 8 == 0 and height % 8 == 0 and pitch % 8 == 0

    def along(axis, size, target, value):
        return lax.ppermute(value, axis, [(i, target(i)) for i in range(size)])

    def across(target, value):
        pairs = [
            (n * blocks + e, target(n) * blocks + (e ^ 1)) for n in range(rows) for e in range(blocks)
        ]
        return lax.ppermute(value, ("north", "east"), pairs)

    shifts = (0, levels - 1, *range(1, levels - 1))
    x = jnp.transpose(pair_rows, (1, 0, 2))
    far = [
        along("east", blocks, lambda e, shift=shift: e ^ (shift * CORES + 1), x)
        for at, shift in enumerate(shifts)
        if at
    ]
    beside = along("east", blocks, lambda e: e ^ 1, x)

    copied = (
        in_gain.reshape(1, channels),
        mid_gain.reshape(1, mix_width),
        left_weight,
        left_gate,
        right_weight,
        right_gate,
        out_weight,
    )
    n = len(copied)
    ready, gate, own_right, turn, gain, mid, lw, lg, rw, rg, ow = call(
        lambda *refs: own_kernel(n, pitch, *refs),
        (
            shape((pairs, channels)),
            shape((pairs, channels), F32),
            shape((pairs, mix_width), F32),
            shape((CORES, pairs, part_rows * pitch)),
            *(shape(a.shape, a.dtype) for a in copied),
        ),
        [HBM] * (2 + n),
        [pltpu.with_memory_space_constraint(a, pltpu.HBM) for a in (x, out_gate, *copied)],
        1.5,
        [
            pltpu.VMEM(x.shape, BF16),
            pltpu.VMEM(out_gate.shape, BF16),
            pltpu.SemaphoreType.DMA((2 + n,)),
        ],
    )

    part = shape((width, both, mix_width))
    flat = pltpu.VMEM((pairs, mix_width), F32)
    right, own_part = call(
        first_kernel,
        (shape((height, both // 8, 8, mix_width), F32), part),
        [VMEM] * 8,
        (beside, gain, lw, lg, rw, rg, ready, own_right),
        1.0,
        [pltpu.VMEM((both * height, mix_width), F32), flat],
    )
    parts = [own_part]
    for s in range(1, levels - 1):
        parts.append(
            call(next_kernel, part, [VMEM] * 5, (far[s - 1], gain, lw, lg, right), 0.6, [flat])
        )
    sums = call(
        lambda *refs: last_kernel(shifts, rows, *refs),
        (shape((part_rows, both, mix_width)),) * rows,
        [VMEM] * (4 + levels),
        (far[-1], gain, lw, lg, right, *parts),
        0.8,
        [pltpu.VMEM((levels, width, both, mix_width), BF16), flat],
    )
    own_sums = along("east", blocks, lambda e: e ^ 1, sums[0])
    arrived = [own_sums] + [across(lambda n, a=a: n ^ a, sums[a]) for a in range(1, rows)]

    half = shape((part_rows, pitch, mix_width))
    scale = (height * rows) ** (-0.5)
    keep, send = call(
        lambda *refs: sum_kernel(scale, *refs),
        (half, half),
        [VMEM] * (1 + rows),
        (mid, *arrived),
        0.3,
    )
    come = along("east", blocks, lambda e: e ^ 1, send)
    kept = call(keep_kernel, shape((pairs, channels), F32), [VMEM] * 3, (keep, turn, ow), 0.3)
    out = call(
        out_kernel, shape((width, height, channels)), [VMEM] * 5, (come, turn, ow, kept, gate), 0.5
    )
    return jnp.transpose(out, (1, 0, 2))


def solution(mesh):
    placed = (P("north", "east", None), P(), P(), P(), P(), P(), P(), P(), P())

    return jax.shard_map(
        body, mesh=mesh, in_specs=placed, out_specs=P("north", "east", None), check_vma=False
    )
```

```python
import math

import jax
import jax.numpy as jnp
from jax import lax
from jax.experimental import pallas as pl
from jax.experimental.pallas import tpu as pltpu
from jax.sharding import PartitionSpec as P


F32, BF16 = jnp.float32, jnp.bfloat16
CORES = 2
VMEM = pl.BlockSpec(memory_space=pltpu.VMEM)
HBM = pl.BlockSpec(memory_space=pltpu.HBM)


def scale_channels(values, channel_gain):
    centred = values - jnp.mean(values, axis=-1, keepdims=True)
    return (
        centred
        * lax.rsqrt(jnp.mean(centred * centred, axis=-1, keepdims=True) + 1e-05)
        * channel_gain
    )


def dot(a, b):
    return jnp.dot(a, b, preferred_element_type=F32)


def shape(dims, dtype=BF16):
    return jax.ShapeDtypeStruct(tuple(dims), dtype)


def call(kernel, outs, specs, args, us, scratch=()):
    tree = jax.tree.map(lambda _: VMEM, outs)
    live = sum(math.prod(a.shape) * a.dtype.itemsize for a in (*jax.tree.leaves(outs), *args))
    live += sum(math.prod(s.shape) * 4 for s in scratch if s.memory_space == pltpu.VMEM)
    return pl.pallas_call(
        kernel,
        out_shape=outs,
        in_specs=specs,
        out_specs=tree,
        scratch_shapes=list(scratch),
        cost_estimate=pl.CostEstimate(flops=int(us * 16e6), bytes_accessed=0, transcendentals=0),
        compiler_params=pltpu.CompilerParams(vmem_limit_bytes=min((8 << 20) + 2 * live, 60 << 20)),
    )(*args)


def ready_of(x_ref, gain):
    width, height, channels = x_ref.shape
    x = x_ref[...].astype(F32).reshape(width * height, channels)
    return scale_channels(x, gain).astype(BF16)


def gated(ready, weight_ref, gate_ref):
    return (dot(ready, weight_ref[...]) * jax.nn.sigmoid(dot(ready, gate_ref[...]))).astype(BF16)


def own_kernel(n_copies, pitch, *refs):
    x_hbm, og_hbm = refs[:2]
    sources = refs[2 : 2 + n_copies]
    ready_ref, gate_ref, right_ref, turn_ref = refs[2 + n_copies : 6 + n_copies]
    copies = refs[6 + n_copies : 6 + 2 * n_copies]
    x_ref, og_ref, sems = refs[6 + 2 * n_copies :]
    moves = [
        pltpu.make_async_copy(source, target, sems.at[i])
        for i, (source, target) in enumerate(
            zip((x_hbm, og_hbm, *sources), (x_ref, og_ref, *copies), strict=True)
        )
    ]
    for move in moves:
        move.start()
    width, height, _ = x_ref.shape
    columns = turn_ref.shape[2]
    level, core = lax.div(lax.axis_index("east"), CORES), lax.rem(lax.axis_index("east"), CORES)
    per_row = height // (CORES * width)
    row = lax.broadcasted_iota(jnp.int32, (height, columns), 0)
    column = lax.broadcasted_iota(jnp.int32, (height, columns), 1)
    for half in range(CORES):
        offset = half * (pitch - width)
        for j in range(width):
            hit = jnp.zeros((height, columns), F32)
            for r in range(per_row):
                near = level == lax.axis_index("north") * per_row + r
                at = jnp.where(near, 1 - core, core) if half == 0 else jnp.where(near, core, 1 - core)
                first = (r * CORES + at) * width
                inside = (row >= first) & (row < first + width)
                same = column == (row - first + r * width) * pitch + (j + offset)
                hit = jnp.where(inside & same, 1.0, hit)
            turn_ref[half, pl.ds(j * height, height), :] = hit.astype(BF16)
    for move in moves:
        move.wait()
    gain_ref, _, _, _, rw_ref, rg_ref, _ = copies
    ready = ready_of(x_ref, gain_ref[...])
    ready_ref[...] = ready
    gate_ref[...] = jax.nn.sigmoid(dot(ready, og_ref[...]))
    right_ref[...] = gated(ready, rw_ref, rg_ref).astype(F32)


def mix(out_ref, left_ref, right_ref):
    height, tiles_j, _, channels = right_ref.shape
    width = out_ref.shape[0]
    tile_j = 3 if tiles_j % 3 == 0 else 1
    tile_i = 12 if width % 12 == 0 else 4
    step = 8
    for i0 in range(0, width, tile_i):
        for j0 in range(0, tiles_j, tile_j):

            def some(kk, total, i0=i0, j0=j0):
                total = list(total)
                for dk in range(step):
                    k = kk * step + dk
                    right = right_ref[k, pl.ds(j0, tile_j)]
                    for i in range(tile_i):
                        start = (i0 + i) * height + k
                        total[i] = total[i] + right * left_ref[pl.ds(start, 8, stride=0), :][None]
                return tuple(total)

            zero = jnp.zeros((tile_j, 8, channels), F32)
            total = lax.fori_loop(0, height // step, some, (zero,) * tile_i, unroll=height <= 24)
            for i in range(tile_i):
                out_ref[i0 + i, pl.ds(j0 * 8, tile_j * 8), :] = (
                    total[i].reshape(tile_j * 8, channels).astype(BF16)
                )


def first_kernel(
    x_ref, gain_ref, lw_ref, lg_ref, rw_ref, rg_ref, ready_ref, own_ref, right_ref, part_ref, flat_ref, left_ref
):
    pairs = own_ref.shape[0]
    height, tiles_j, _, channels = right_ref.shape
    other = gated(ready_of(x_ref, gain_ref[...]), rw_ref, rg_ref)
    flat_ref[pl.ds(0, pairs), :] = other.astype(F32)
    flat_ref[pl.ds(pairs, pairs), :] = own_ref[...]
    for k in range(height):
        right_ref[k] = flat_ref[pl.ds(k, tiles_j * 8, stride=height), :].reshape(tiles_j, 8, channels)
    left_ref[...] = gated(ready_ref[...], lw_ref, lg_ref).astype(F32)
    mix(part_ref, left_ref, right_ref)


def next_kernel(x_ref, gain_ref, lw_ref, lg_ref, right_ref, part_ref, left_ref):
    left_ref[...] = gated(ready_of(x_ref, gain_ref[...]), lw_ref, lg_ref).astype(F32)
    mix(part_ref, left_ref, right_ref)


def step_between(level, target, levels):
    def place(z):
        return lax.div(z, 2) + lax.rem(z, 2) * (levels // 2)

    return lax.rem(place(target) - place(level) + levels, levels)


def last_kernel(levels, rows, *refs):
    x_ref, gain_ref, lw_ref, lg_ref, right_ref = refs[:5]
    parts = refs[5 : 4 + levels]
    outs = refs[4 + levels : 4 + levels + rows]
    all_ref, left_ref = refs[4 + levels + rows :]
    level, row = lax.div(lax.axis_index("east"), CORES), lax.axis_index("north")
    left_ref[...] = gated(ready_of(x_ref, gain_ref[...]), lw_ref, lg_ref).astype(F32)
    mix(all_ref.at[levels - 1], left_ref, right_ref)
    for s, ref in enumerate(parts):
        all_ref[s] = ref[...]
    per_row = levels // rows
    width = all_ref.shape[1]
    for a, out_ref in enumerate(outs):
        for r in range(per_row):
            s = step_between(level, (row ^ a) * per_row + r, levels)
            out_ref[pl.ds(r * width, width)] = all_ref[s]


def sum_kernel(scale, gain_ref, *refs):
    parts, (keep_ref, send_ref) = refs[:-2], refs[-2:]
    total = parts[0][...].astype(F32)
    for ref in parts[1:]:
        total = total + ref[...].astype(F32)
    mixed = (total * scale).astype(BF16).astype(F32)
    channels = mixed.shape[2]
    scaled = scale_channels(mixed, gain_ref[...].reshape(1, 1, channels)).astype(BF16)
    pitch = keep_ref.shape[1]
    keep_ref[...] = scaled[:, :pitch]
    send_ref[...] = scaled[:, scaled.shape[1] - pitch :]


def turned(half_ref, turn_ref, which, weight_ref):
    rows, pitch, channels = half_ref.shape
    half = half_ref[...].reshape(rows * pitch, channels)
    return dot(dot(turn_ref[which], half).astype(BF16), weight_ref[...])


def keep_kernel(keep_ref, turn_ref, weight_ref, out_ref):
    out_ref[...] = turned(keep_ref, turn_ref, 0, weight_ref)


def out_kernel(come_ref, turn_ref, weight_ref, kept_ref, gate_ref, out_ref):
    out = (kept_ref[...] + turned(come_ref, turn_ref, 1, weight_ref)) * gate_ref[...]
    out_ref[...] = out.astype(BF16).reshape(out_ref.shape)


def body(
    pair_rows,
    in_gain,
    left_weight,
    right_weight,
    left_gate,
    right_gate,
    mid_gain,
    out_weight,
    out_gate,
):
    rows, blocks = lax.axis_size("north"), lax.axis_size("east")
    levels = blocks // CORES
    per_row = levels // rows
    height, width, channels = pair_rows.shape
    mix_width = left_weight.shape[1]
    both, pairs, part_rows = CORES * width, width * height, per_row * width
    pitch = both - width // 8 * 8
    assert levels == per_row * rows and rows & (rows - 1) == 0 and levels % 2 == 0 and height == per_row * both
    assert both % 8 == 0 and height % 8 == 0 and pitch % 8 == 0

    def along(axes, moves, value):
        return lax.ppermute(value, axes, moves)

    cores = [(e, e ^ 1) for e in range(blocks)]

    circle = [*range(0, levels, 2), *range(1, levels, 2)]

    def source(level, s):
        return circle[(circle.index(level) + s) % levels]

    x = jnp.transpose(pair_rows, (1, 0, 2))
    far = [
        along(
            "east",
            [
                (source(e // CORES, s) * CORES + (1 - e % CORES), e)
                for e in range(blocks)
            ],
            x,
        )
        for s in range(1, levels)
    ]
    beside = along("east", cores, x)

    copied = (
        in_gain.reshape(1, channels),
        mid_gain.reshape(1, mix_width),
        left_weight,
        left_gate,
        right_weight,
        right_gate,
        out_weight,
    )
    n = len(copied)
    ready, gate, own_right, turn, gain, mid, lw, lg, rw, rg, ow = call(
        lambda *refs: own_kernel(n, pitch, *refs),
        (
            shape((pairs, channels)),
            shape((pairs, channels), F32),
            shape((pairs, mix_width), F32),
            shape((CORES, pairs, part_rows * pitch)),
            *(shape(a.shape, a.dtype) for a in copied),
        ),
        [HBM] * (2 + n),
        [pltpu.with_memory_space_constraint(a, pltpu.HBM) for a in (x, out_gate, *copied)],
        1.5,
        [
            pltpu.VMEM(x.shape, BF16),
            pltpu.VMEM(out_gate.shape, BF16),
            pltpu.SemaphoreType.DMA((2 + n,)),
        ],
    )

    part = shape((width, both, mix_width))
    flat = pltpu.VMEM((pairs, mix_width), F32)
    right, own_part = call(
        first_kernel,
        (shape((height, both // 8, 8, mix_width), F32), part),
        [VMEM] * 8,
        (beside, gain, lw, lg, rw, rg, ready, own_right),
        1.0,
        [pltpu.VMEM((both * height, mix_width), F32), flat],
    )
    parts = [own_part]
    for s in range(1, levels - 1):
        parts.append(
            call(next_kernel, part, [VMEM] * 5, (far[s - 1], gain, lw, lg, right), 0.6, [flat])
        )
    sums = call(
        lambda *refs: last_kernel(levels, rows, *refs),
        (shape((part_rows, both, mix_width)),) * rows,
        [VMEM] * (4 + levels),
        (far[-1], gain, lw, lg, right, *parts),
        0.8,
        [pltpu.VMEM((levels, width, both, mix_width), BF16), flat],
    )
    arrived = [along("east", cores, sums[0])]
    for a in range(1, rows):
        moves = [
            (n * blocks + e, (n ^ a) * blocks + (e ^ 1)) for n in range(rows) for e in range(blocks)
        ]
        arrived.append(along(("north", "east"), moves, sums[a]))

    half = shape((part_rows, pitch, mix_width))
    scale = (height * rows) ** (-0.5)
    keep, send = call(
        lambda *refs: sum_kernel(scale, *refs),
        (half, half),
        [VMEM] * (1 + rows),
        (mid, *arrived),
        0.3,
    )
    come = along("east", cores, send)
    kept = call(keep_kernel, shape((pairs, channels), F32), [VMEM] * 3, (keep, turn, ow), 0.3)
    out = call(
        out_kernel, shape((width, height, channels)), [VMEM] * 5, (come, turn, ow, kept, gate), 0.5
    )
    return jnp.transpose(out, (1, 0, 2))


def solution(mesh):
    placed = (P("north", "east", None), P(), P(), P(), P(), P(), P(), P(), P())

    return jax.shard_map(
        body, mesh=mesh, in_specs=placed, out_specs=P("north", "east", None), check_vma=False
    )
```

```python
import math

import jax
import jax.numpy as jnp
from jax import lax
from jax.experimental import pallas as pl
from jax.experimental.pallas import tpu as pltpu
from jax.sharding import PartitionSpec as P


F32, BF16 = jnp.float32, jnp.bfloat16
CORES = 2
VMEM = pl.BlockSpec(memory_space=pltpu.VMEM)
HBM = pl.BlockSpec(memory_space=pltpu.HBM)


def scale_channels(values, channel_gain):
    centred = values - jnp.mean(values, axis=-1, keepdims=True)
    return (
        centred
        * lax.rsqrt(jnp.mean(centred * centred, axis=-1, keepdims=True) + 1e-05)
        * channel_gain
    )


def dot(a, b):
    return jnp.dot(a, b, preferred_element_type=F32)


def shape(dims, dtype=BF16):
    return jax.ShapeDtypeStruct(tuple(dims), dtype)


def call(kernel, outs, specs, args, us, scratch=()):
    tree = jax.tree.map(lambda _: VMEM, outs)
    live = sum(math.prod(a.shape) * a.dtype.itemsize for a in (*jax.tree.leaves(outs), *args))
    live += sum(math.prod(s.shape) * 4 for s in scratch if s.memory_space == pltpu.VMEM)
    return pl.pallas_call(
        kernel,
        out_shape=outs,
        in_specs=specs,
        out_specs=tree,
        scratch_shapes=list(scratch),
        cost_estimate=pl.CostEstimate(flops=int(us * 16e6), bytes_accessed=0, transcendentals=0),
        compiler_params=pltpu.CompilerParams(vmem_limit_bytes=min((8 << 20) + 2 * live, 60 << 20)),
    )(*args)


def ready_of(x_ref, gain):
    width, height, channels = x_ref.shape
    x = x_ref[...].astype(F32).reshape(width * height, channels)
    return scale_channels(x, gain).astype(BF16)


def gated(ready, weight_ref, gate_ref):
    return (dot(ready, weight_ref[...]) * jax.nn.sigmoid(dot(ready, gate_ref[...]))).astype(BF16)


def own_kernel(n_copies, pitch, *refs):
    x_hbm, og_hbm = refs[:2]
    sources = refs[2 : 2 + n_copies]
    ready_ref, gate_ref, right_ref, turn_ref = refs[2 + n_copies : 6 + n_copies]
    copies = refs[6 + n_copies : 6 + 2 * n_copies]
    x_ref, og_ref, sems = refs[6 + 2 * n_copies :]
    moves = [
        pltpu.make_async_copy(source, target, sems.at[i])
        for i, (source, target) in enumerate(
            zip((x_hbm, og_hbm, *sources), (x_ref, og_ref, *copies), strict=True)
        )
    ]
    for move in moves:
        move.start()
    width, height, _ = x_ref.shape
    columns = turn_ref.shape[2]
    level, core = lax.div(lax.axis_index("east"), CORES), lax.rem(lax.axis_index("east"), CORES)
    per_row = height // (CORES * width)
    row = lax.broadcasted_iota(jnp.int32, (height, columns), 0)
    column = lax.broadcasted_iota(jnp.int32, (height, columns), 1)
    for half in range(CORES):
        offset = half * (pitch - width)
        for j in range(width):
            hit = jnp.zeros((height, columns), F32)
            for r in range(per_row):
                near = level == lax.axis_index("north") * per_row + r
                at = jnp.where(near, 1 - core, core) if half == 0 else jnp.where(near, core, 1 - core)
                first = (r * CORES + at) * width
                inside = (row >= first) & (row < first + width)
                same = column == (row - first + r * width) * pitch + (j + offset)
                hit = jnp.where(inside & same, 1.0, hit)
            turn_ref[half, pl.ds(j * height, height), :] = hit.astype(BF16)
    for move in moves:
        move.wait()
    gain_ref, _, _, _, rw_ref, rg_ref, _ = copies
    ready = ready_of(x_ref, gain_ref[...])
    ready_ref[...] = ready
    gate_ref[...] = jax.nn.sigmoid(dot(ready, og_ref[...]))
    right_ref[...] = gated(ready, rw_ref, rg_ref).astype(F32)


def mix(out_ref, left_ref, right_ref):
    height, tiles_j, _, channels = right_ref.shape
    width = out_ref.shape[0]
    tile_j = 3 if tiles_j % 3 == 0 else 1
    tile_i = 12 if width % 12 == 0 else 4
    step = 8
    for i0 in range(0, width, tile_i):
        for j0 in range(0, tiles_j, tile_j):

            def some(kk, total, i0=i0, j0=j0):
                total = list(total)
                for dk in range(step):
                    k = kk * step + dk
                    right = right_ref[k, pl.ds(j0, tile_j)]
                    for i in range(tile_i):
                        start = (i0 + i) * height + k
                        total[i] = total[i] + right * left_ref[pl.ds(start, 8, stride=0), :][None]
                return tuple(total)

            zero = jnp.zeros((tile_j, 8, channels), F32)
            total = lax.fori_loop(0, height // step, some, (zero,) * tile_i, unroll=height <= 24)
            for i in range(tile_i):
                out_ref[i0 + i, pl.ds(j0 * 8, tile_j * 8), :] = (
                    total[i].reshape(tile_j * 8, channels).astype(BF16)
                )


def first_kernel(
    x_ref, gain_ref, lw_ref, lg_ref, rw_ref, rg_ref, ready_ref, own_ref, right_ref, part_ref, flat_ref, left_ref
):
    pairs = own_ref.shape[0]
    height, tiles_j, _, channels = right_ref.shape
    other = gated(ready_of(x_ref, gain_ref[...]), rw_ref, rg_ref)
    flat_ref[pl.ds(0, pairs), :] = other.astype(F32)
    flat_ref[pl.ds(pairs, pairs), :] = own_ref[...]
    for k in range(height):
        right_ref[k] = flat_ref[pl.ds(k, tiles_j * 8, stride=height), :].reshape(tiles_j, 8, channels)
    left_ref[...] = gated(ready_ref[...], lw_ref, lg_ref).astype(F32)
    mix(part_ref, left_ref, right_ref)


def next_kernel(x_ref, gain_ref, lw_ref, lg_ref, right_ref, part_ref, left_ref):
    left_ref[...] = gated(ready_of(x_ref, gain_ref[...]), lw_ref, lg_ref).astype(F32)
    mix(part_ref, left_ref, right_ref)


def owner(row, a, rows):
    circle = [place ^ (place >> 1) for place in range(rows)]
    return circle[(circle.index(row) + a) % rows]


def step_between(level, target, levels):
    def place(z):
        return lax.div(z, 2) + lax.rem(z, 2) * (levels // 2)

    return lax.rem(place(target) - place(level) + levels, levels)


def last_kernel(levels, rows, *refs):
    x_ref, gain_ref, lw_ref, lg_ref, right_ref = refs[:5]
    parts = refs[5 : 4 + levels]
    outs = refs[4 + levels : 4 + levels + rows]
    all_ref, left_ref = refs[4 + levels + rows :]
    level, row = lax.div(lax.axis_index("east"), CORES), lax.axis_index("north")
    left_ref[...] = gated(ready_of(x_ref, gain_ref[...]), lw_ref, lg_ref).astype(F32)
    mix(all_ref.at[levels - 1], left_ref, right_ref)
    for s, ref in enumerate(parts):
        all_ref[s] = ref[...]
    per_row = levels // rows
    width = all_ref.shape[1]
    for a, out_ref in enumerate(outs):
        for r in range(per_row):
            to = sum(jnp.where(row == n, owner(n, a, rows), 0) for n in range(rows))
            s = step_between(level, to * per_row + r, levels)
            out_ref[pl.ds(r * width, width)] = all_ref[s]


def sum_kernel(scale, gain_ref, *refs):
    parts, (keep_ref, send_ref) = refs[:-2], refs[-2:]
    total = parts[0][...].astype(F32)
    for ref in parts[1:]:
        total = total + ref[...].astype(F32)
    mixed = (total * scale).astype(BF16).astype(F32)
    channels = mixed.shape[2]
    scaled = scale_channels(mixed, gain_ref[...].reshape(1, 1, channels)).astype(BF16)
    pitch = keep_ref.shape[1]
    keep_ref[...] = scaled[:, :pitch]
    send_ref[...] = scaled[:, scaled.shape[1] - pitch :]


def turned(half_ref, turn_ref, which, weight_ref):
    rows, pitch, channels = half_ref.shape
    half = half_ref[...].reshape(rows * pitch, channels)
    return dot(dot(turn_ref[which], half).astype(BF16), weight_ref[...])


def keep_kernel(keep_ref, turn_ref, weight_ref, out_ref):
    out_ref[...] = turned(keep_ref, turn_ref, 0, weight_ref)


def out_kernel(come_ref, turn_ref, weight_ref, kept_ref, gate_ref, out_ref):
    out = (kept_ref[...] + turned(come_ref, turn_ref, 1, weight_ref)) * gate_ref[...]
    out_ref[...] = out.astype(BF16).reshape(out_ref.shape)


def body(
    pair_rows,
    in_gain,
    left_weight,
    right_weight,
    left_gate,
    right_gate,
    mid_gain,
    out_weight,
    out_gate,
):
    rows, blocks = lax.axis_size("north"), lax.axis_size("east")
    levels = blocks // CORES
    per_row = levels // rows
    height, width, channels = pair_rows.shape
    mix_width = left_weight.shape[1]
    both, pairs, part_rows = CORES * width, width * height, per_row * width
    pitch = both - width // 8 * 8
    assert levels == per_row * rows and rows & (rows - 1) == 0 and levels % 2 == 0 and height == per_row * both
    assert both % 8 == 0 and height % 8 == 0 and pitch % 8 == 0

    def along(axes, moves, value):
        return lax.ppermute(value, axes, moves)

    cores = [(e, e ^ 1) for e in range(blocks)]

    circle = [*range(0, levels, 2), *range(1, levels, 2)]

    def source(level, s):
        return circle[(circle.index(level) + s) % levels]

    x = jnp.transpose(pair_rows, (1, 0, 2))
    far = [
        along(
            "east",
            [
                (source(e // CORES, s) * CORES + (1 - e % CORES), e)
                for e in range(blocks)
            ],
            x,
        )
        for s in range(1, levels)
    ]
    beside = along("east", cores, x)

    copied = (
        in_gain.reshape(1, channels),
        mid_gain.reshape(1, mix_width),
        left_weight,
        left_gate,
        right_weight,
        right_gate,
        out_weight,
    )
    n = len(copied)
    ready, gate, own_right, turn, gain, mid, lw, lg, rw, rg, ow = call(
        lambda *refs: own_kernel(n, pitch, *refs),
        (
            shape((pairs, channels)),
            shape((pairs, channels), F32),
            shape((pairs, mix_width), F32),
            shape((CORES, pairs, part_rows * pitch)),
            *(shape(a.shape, a.dtype) for a in copied),
        ),
        [HBM] * (2 + n),
        [pltpu.with_memory_space_constraint(a, pltpu.HBM) for a in (x, out_gate, *copied)],
        1.5,
        [
            pltpu.VMEM(x.shape, BF16),
            pltpu.VMEM(out_gate.shape, BF16),
            pltpu.SemaphoreType.DMA((2 + n,)),
        ],
    )

    part = shape((width, both, mix_width))
    flat = pltpu.VMEM((pairs, mix_width), F32)
    right, own_part = call(
        first_kernel,
        (shape((height, both // 8, 8, mix_width), F32), part),
        [VMEM] * 8,
        (beside, gain, lw, lg, rw, rg, ready, own_right),
        1.0,
        [pltpu.VMEM((both * height, mix_width), F32), flat],
    )
    parts = [own_part]
    for s in range(1, levels - 1):
        parts.append(
            call(next_kernel, part, [VMEM] * 5, (far[s - 1], gain, lw, lg, right), 0.6, [flat])
        )
    sums = call(
        lambda *refs: last_kernel(levels, rows, *refs),
        (shape((part_rows, both, mix_width)),) * rows,
        [VMEM] * (4 + levels),
        (far[-1], gain, lw, lg, right, *parts),
        0.8,
        [pltpu.VMEM((levels, width, both, mix_width), BF16), flat],
    )
    arrived = [along("east", cores, sums[0])]
    for a in range(1, rows):
        moves = [
            (n * blocks + e, owner(n, a, rows) * blocks + (e ^ 1))
            for n in range(rows)
            for e in range(blocks)
        ]
        arrived.append(along(("north", "east"), moves, sums[a]))

    half = shape((part_rows, pitch, mix_width))
    scale = (height * rows) ** (-0.5)
    keep, send = call(
        lambda *refs: sum_kernel(scale, *refs),
        (half, half),
        [VMEM] * (1 + rows),
        (mid, *arrived),
        0.3,
    )
    come = along("east", cores, send)
    kept = call(keep_kernel, shape((pairs, channels), F32), [VMEM] * 3, (keep, turn, ow), 0.3)
    out = call(
        out_kernel, shape((width, height, channels)), [VMEM] * 5, (come, turn, ow, kept, gate), 0.5
    )
    return jnp.transpose(out, (1, 0, 2))


def solution(mesh):
    placed = (P("north", "east", None), P(), P(), P(), P(), P(), P(), P(), P())

    return jax.shard_map(
        body, mesh=mesh, in_specs=placed, out_specs=P("north", "east", None), check_vma=False
    )
```

```python
import math

import jax
import jax.numpy as jnp
from jax import lax
from jax.experimental import pallas as pl
from jax.experimental.pallas import tpu as pltpu
from jax.sharding import PartitionSpec as P


F32, BF16 = jnp.float32, jnp.bfloat16
CORES = 2
VMEM = pl.BlockSpec(memory_space=pltpu.VMEM)
HBM = pl.BlockSpec(memory_space=pltpu.HBM)


def scale_channels(values, channel_gain):
    centred = values - jnp.mean(values, axis=-1, keepdims=True)
    return (
        centred
        * lax.rsqrt(jnp.mean(centred * centred, axis=-1, keepdims=True) + 1e-05)
        * channel_gain
    )


def dot(a, b):
    return jnp.dot(a, b, preferred_element_type=F32)


def shape(dims, dtype=BF16):
    return jax.ShapeDtypeStruct(tuple(dims), dtype)


def call(kernel, outs, specs, args, us, scratch=()):
    tree = jax.tree.map(lambda _: VMEM, outs)
    live = sum(math.prod(a.shape) * a.dtype.itemsize for a in (*jax.tree.leaves(outs), *args))
    live += sum(math.prod(s.shape) * 4 for s in scratch if s.memory_space == pltpu.VMEM)
    return pl.pallas_call(
        kernel,
        out_shape=outs,
        in_specs=specs,
        out_specs=tree,
        scratch_shapes=list(scratch),
        cost_estimate=pl.CostEstimate(flops=int(us * 16e6), bytes_accessed=0, transcendentals=0),
        compiler_params=pltpu.CompilerParams(vmem_limit_bytes=min((8 << 20) + 2 * live, 60 << 20)),
    )(*args)


def ready_of(x_ref, gain):
    width, height, channels = x_ref.shape
    x = x_ref[...].astype(F32).reshape(width * height, channels)
    return scale_channels(x, gain).astype(BF16)


def gated(ready, weight_ref, gate_ref):
    return (dot(ready, weight_ref[...]) * jax.nn.sigmoid(dot(ready, gate_ref[...]))).astype(BF16)


def own_kernel(n_copies, pitch, *refs):
    x_hbm, og_hbm = refs[:2]
    sources = refs[2 : 2 + n_copies]
    ready_ref, gate_ref, right_ref, turn_ref = refs[2 + n_copies : 6 + n_copies]
    copies = refs[6 + n_copies : 6 + 2 * n_copies]
    x_ref, og_ref, sems = refs[6 + 2 * n_copies :]
    moves = [
        pltpu.make_async_copy(source, target, sems.at[i])
        for i, (source, target) in enumerate(
            zip((x_hbm, og_hbm, *sources), (x_ref, og_ref, *copies), strict=True)
        )
    ]
    for move in moves:
        move.start()
    width, height, _ = x_ref.shape
    columns = turn_ref.shape[2]
    level, core = lax.div(lax.axis_index("east"), CORES), lax.rem(lax.axis_index("east"), CORES)
    per_row = height // (CORES * width)
    row = lax.broadcasted_iota(jnp.int32, (height, columns), 0)
    column = lax.broadcasted_iota(jnp.int32, (height, columns), 1)
    for half in range(CORES):
        offset = half * (pitch - width)
        for j in range(width):
            hit = jnp.zeros((height, columns), F32)
            for r in range(per_row):
                near = level == lax.axis_index("north") * per_row + r
                at = jnp.where(near, 1 - core, core) if half == 0 else jnp.where(near, core, 1 - core)
                first = (r * CORES + at) * width
                inside = (row >= first) & (row < first + width)
                same = column == (row - first + r * width) * pitch + (j + offset)
                hit = jnp.where(inside & same, 1.0, hit)
            turn_ref[half, pl.ds(j * height, height), :] = hit.astype(BF16)
    for move in moves:
        move.wait()
    gain_ref, _, _, _, rw_ref, rg_ref, _ = copies
    ready = ready_of(x_ref, gain_ref[...])
    ready_ref[...] = ready
    gate_ref[...] = jax.nn.sigmoid(dot(ready, og_ref[...]))
    right_ref[...] = gated(ready, rw_ref, rg_ref).astype(F32)


def mix(out_ref, left_ref, right_ref):
    height, tiles_j, _, channels = right_ref.shape
    width = out_ref.shape[0]
    tile_j = 3 if tiles_j % 3 == 0 else 1
    tile_i = 12 if width % 12 == 0 else 4
    step = 8
    for i0 in range(0, width, tile_i):
        for j0 in range(0, tiles_j, tile_j):

            def some(kk, total, i0=i0, j0=j0):
                total = list(total)
                for dk in range(step):
                    k = kk * step + dk
                    right = right_ref[k, pl.ds(j0, tile_j)]
                    for i in range(tile_i):
                        start = (i0 + i) * height + k
                        total[i] = total[i] + right * left_ref[pl.ds(start, 8, stride=0), :][None]
                return tuple(total)

            zero = jnp.zeros((tile_j, 8, channels), F32)
            total = lax.fori_loop(0, height // step, some, (zero,) * tile_i, unroll=height <= 24)
            for i in range(tile_i):
                out_ref[i0 + i, pl.ds(j0 * 8, tile_j * 8), :] = (
                    total[i].reshape(tile_j * 8, channels).astype(BF16)
                )


def first_kernel(
    x_ref, gain_ref, lw_ref, lg_ref, rw_ref, rg_ref, ready_ref, own_ref, right_ref, part_ref, flat_ref, left_ref
):
    pairs = own_ref.shape[0]
    height, tiles_j, _, channels = right_ref.shape
    other = gated(ready_of(x_ref, gain_ref[...]), rw_ref, rg_ref)
    flat_ref[pl.ds(0, pairs), :] = other.astype(F32)
    flat_ref[pl.ds(pairs, pairs), :] = own_ref[...]
    for k in range(height):
        right_ref[k] = flat_ref[pl.ds(k, tiles_j * 8, stride=height), :].reshape(tiles_j, 8, channels)
    left_ref[...] = gated(ready_ref[...], lw_ref, lg_ref).astype(F32)
    mix(part_ref, left_ref, right_ref)


def next_kernel(x_ref, gain_ref, lw_ref, lg_ref, right_ref, part_ref, left_ref):
    left_ref[...] = gated(ready_of(x_ref, gain_ref[...]), lw_ref, lg_ref).astype(F32)
    mix(part_ref, left_ref, right_ref)


def step_between(level, target, levels):
    def place(z):
        return lax.div(z, 2) + lax.rem(z, 2) * (levels // 2)

    return lax.rem(place(target) - place(level) + levels, levels)


def last_kernel(levels, rows, *refs):
    x_ref, gain_ref, lw_ref, lg_ref, right_ref = refs[:5]
    parts = refs[5 : 4 + levels]
    outs = refs[4 + levels : 4 + levels + rows]
    all_ref, left_ref = refs[4 + levels + rows :]
    level, row = lax.div(lax.axis_index("east"), CORES), lax.axis_index("north")
    left_ref[...] = gated(ready_of(x_ref, gain_ref[...]), lw_ref, lg_ref).astype(F32)
    mix(all_ref.at[levels - 1], left_ref, right_ref)
    for s, ref in enumerate(parts):
        all_ref[s] = ref[...]
    per_row = levels // rows
    width = all_ref.shape[1]
    for a, out_ref in enumerate(outs):
        for r in range(per_row):
            s = step_between(level, (row ^ a) * per_row + r, levels)
            out_ref[pl.ds(r * width, width)] = all_ref[s]


def sum_kernel(scale, gain_ref, weight_ref, *refs):
    parts, (keep_ref, send_ref) = refs[:-2], refs[-2:]
    total = parts[0][...].astype(F32)
    for ref in parts[1:]:
        total = total + ref[...].astype(F32)
    mixed = (total * scale).astype(BF16).astype(F32)
    rows, _, channels = mixed.shape
    scaled = scale_channels(mixed, gain_ref[...].reshape(1, 1, channels)).astype(BF16)
    pitch = keep_ref.shape[1]
    keep_ref[...] = scaled[:, :pitch]
    half = scaled[:, scaled.shape[1] - pitch :].reshape(rows * pitch, channels)
    send_ref[...] = dot(half, weight_ref[...]).astype(BF16).reshape(send_ref.shape)


def turned(half_ref, turn_ref, which, weight_ref):
    rows, pitch, channels = half_ref.shape
    half = half_ref[...].reshape(rows * pitch, channels)
    return dot(dot(turn_ref[which], half).astype(BF16), weight_ref[...])


def keep_kernel(keep_ref, turn_ref, weight_ref, out_ref):
    out_ref[...] = turned(keep_ref, turn_ref, 0, weight_ref)


def out_kernel(come_ref, turn_ref, kept_ref, gate_ref, out_ref):
    rows, pitch, channels = come_ref.shape
    come = come_ref[...].reshape(rows * pitch, channels)
    out = (kept_ref[...] + dot(turn_ref[1], come)) * gate_ref[...]
    out_ref[...] = out.astype(BF16).reshape(out_ref.shape)


def body(
    pair_rows,
    in_gain,
    left_weight,
    right_weight,
    left_gate,
    right_gate,
    mid_gain,
    out_weight,
    out_gate,
):
    rows, blocks = lax.axis_size("north"), lax.axis_size("east")
    levels = blocks // CORES
    per_row = levels // rows
    height, width, channels = pair_rows.shape
    mix_width = left_weight.shape[1]
    both, pairs, part_rows = CORES * width, width * height, per_row * width
    pitch = both - width // 8 * 8
    assert levels == per_row * rows and rows & (rows - 1) == 0 and levels % 2 == 0 and height == per_row * both
    assert both % 8 == 0 and height % 8 == 0 and pitch % 8 == 0

    def along(axes, moves, value):
        return lax.ppermute(value, axes, moves)

    cores = [(e, e ^ 1) for e in range(blocks)]

    circle = [*range(0, levels, 2), *range(1, levels, 2)]

    def source(level, s):
        return circle[(circle.index(level) + s) % levels]

    x = jnp.transpose(pair_rows, (1, 0, 2))
    far = [
        along(
            "east",
            [
                (source(e // CORES, s) * CORES + (1 - e % CORES), e)
                for e in range(blocks)
            ],
            x,
        )
        for s in range(1, levels)
    ]
    beside = along("east", cores, x)

    copied = (
        in_gain.reshape(1, channels),
        mid_gain.reshape(1, mix_width),
        left_weight,
        left_gate,
        right_weight,
        right_gate,
        out_weight,
    )
    n = len(copied)
    ready, gate, own_right, turn, gain, mid, lw, lg, rw, rg, ow = call(
        lambda *refs: own_kernel(n, pitch, *refs),
        (
            shape((pairs, channels)),
            shape((pairs, channels), F32),
            shape((pairs, mix_width), F32),
            shape((CORES, pairs, part_rows * pitch)),
            *(shape(a.shape, a.dtype) for a in copied),
        ),
        [HBM] * (2 + n),
        [pltpu.with_memory_space_constraint(a, pltpu.HBM) for a in (x, out_gate, *copied)],
        1.5,
        [
            pltpu.VMEM(x.shape, BF16),
            pltpu.VMEM(out_gate.shape, BF16),
            pltpu.SemaphoreType.DMA((2 + n,)),
        ],
    )

    part = shape((width, both, mix_width))
    flat = pltpu.VMEM((pairs, mix_width), F32)
    right, own_part = call(
        first_kernel,
        (shape((height, both // 8, 8, mix_width), F32), part),
        [VMEM] * 8,
        (beside, gain, lw, lg, rw, rg, ready, own_right),
        1.0,
        [pltpu.VMEM((both * height, mix_width), F32), flat],
    )
    parts = [own_part]
    for s in range(1, levels - 1):
        parts.append(
            call(next_kernel, part, [VMEM] * 5, (far[s - 1], gain, lw, lg, right), 0.6, [flat])
        )
    sums = call(
        lambda *refs: last_kernel(levels, rows, *refs),
        (shape((part_rows, both, mix_width)),) * rows,
        [VMEM] * (4 + levels),
        (far[-1], gain, lw, lg, right, *parts),
        0.8,
        [pltpu.VMEM((levels, width, both, mix_width), BF16), flat],
    )
    arrived = [along("east", cores, sums[0])]
    for a in range(1, rows):
        moves = [
            (n * blocks + e, (n ^ a) * blocks + (e ^ 1)) for n in range(rows) for e in range(blocks)
        ]
        arrived.append(along(("north", "east"), moves, sums[a]))

    half = shape((part_rows, pitch, mix_width))
    scale = (height * rows) ** (-0.5)
    keep, send = call(
        lambda *refs: sum_kernel(scale, *refs),
        (half, shape((part_rows, pitch, channels))),
        [VMEM] * (2 + rows),
        (mid, ow, *arrived),
        0.3,
    )
    come = along("east", cores, send)
    kept = call(keep_kernel, shape((pairs, channels), F32), [VMEM] * 3, (keep, turn, ow), 0.3)
    out = call(
        out_kernel, shape((width, height, channels)), [VMEM] * 4, (come, turn, kept, gate), 0.5
    )
    return jnp.transpose(out, (1, 0, 2))


def solution(mesh):
    placed = (P("north", "east", None), P(), P(), P(), P(), P(), P(), P(), P())

    return jax.shard_map(
        body, mesh=mesh, in_specs=placed, out_specs=P("north", "east", None), check_vma=False
    )
```
